256 devices in a mesh: dp: 64 (over x, y, z_hi, core), mp: 4 (over z_lo).
Axes of the slice: x: 4, y: 4, z: 8 (z_hi: 2, z_lo: 4; z = z_hi * 4 + z_lo), core: 2. Of those that a mesh axis runs over, the one named last changes fastest.
Arguments:
- states: bfloat16 [1024, 80, 768], P('dp'), may hold values from -16 to 16
- hist_len: int32 [1024], P('dp'), may hold values from 1 to 20
- norm_gain: float32 [768], replicated, may hold values from 0.5 to 1.5
- qkv_weight: bfloat16 [768, 3, 12, 64], P(None, None, 'mp'), may hold values from -1 to 1
- output_weight: bfloat16 [12, 64, 768], P('mp'), may hold values from -0.21875 to 0.21875
- cotangent: bfloat16 [1024, 80, 768], P('dp'), may hold values from -16 to 16
Outputs:
- attended: bfloat16 [1024, 80, 768], P('dp')
- grad_states: bfloat16 [1024, 80, 768], P('dp')
- grad_qkv: float32 [768, 3, 12, 64], P('dp', None, 'mp')
- output_weight_gradient: float32 [12, 64, 768], P('mp', None, 'dp')
- grad_gain: float32 [768], P('dp')
The draws below stay inside these ranges and needn't reach their ends.
All inputs are finite; a program needn't handle non-finite values.
Results may differ from the reference program's by a relative error of at most 0.012.
Values may be sent and summed in bfloat16 or wider, within the bound.
A program may use at most 128 MiB of HBM per device.

```python
import jax
import jax.numpy as jnp
from jax import lax

D = 768
H = 12
DH = 64
ITEMS = 20
LEVELS = 4
S = 80
B = 1024


def draw_qkv_weight(key, part):
    k_base, k_noise, k_value = jax.random.split(key, 3)
    inverse = D ** (-0.5)
    query_part = 0.5 * inverse * jax.random.normal(k_base, (D, H, DH), jnp.float32)
    key_part = 0.5 * inverse * jax.random.normal(k_noise, (D, H, DH), jnp.float32)
    value_part = inverse * jax.random.normal(k_value, (D, H, DH), jnp.float32)
    stacked = jnp.stack([query_part, key_part, value_part], axis=1)
    return jnp.clip(stacked, -1.0, 1.0).astype(jnp.bfloat16)


def set_ends(drawn, own_key, least, high):
    longest = drawn.shape.index(max(drawn.shape))
    spots = []
    for shift in (0, 1):
        where = [jax.random.randint(jax.random.fold_in(own_key, axis), (), 0, length) for axis, length in enumerate(drawn.shape)]
        where[longest] = (where[longest] + shift) % drawn.shape[longest]
        spots.append(tuple(where))
    return drawn.at[spots[0]].set(least).at[spots[1]].set(high)


def with_spikes(drawn, key, source, target, blocks, factor):
    def block_of(dim):
        return (jnp.arange(drawn.shape[dim]) // (drawn.shape[dim] // blocks)).reshape((-1,) + (1,) * (drawn.ndim - 1 - dim))

    first = jax.random.permutation(key, blocks)[block_of(target)]
    far = (block_of(target) + blocks // 2) % blocks
    return jnp.where((block_of(source) == first) | (block_of(source) == far), factor * drawn, drawn)


def block_levels(stream_key, extent, cuts, smallest, high):
    level, own = 1.0, jax.random.fold_in(stream_key, 6)
    for dim, blocks in cuts:
        heights = jnp.exp(jax.random.uniform(jax.random.fold_in(own, dim), (blocks,), jnp.float32, smallest / len(cuts), high / len(cuts)))
        level = level * jnp.repeat(heights, extent[dim] // blocks).reshape([-1 if axis == dim else 1 for axis in range(len(extent))])
    return level


def gaussian(own_key, shape, deviation, limit, pieces=(), kind=jnp.bfloat16):
    array = jax.random.normal(own_key, shape, jnp.float32) * deviation
    if len(pieces) > 0:
        array = block_levels(own_key, shape, pieces, -0.22, 0.18) * array
    return jnp.clip(array, min=-limit, max=limit).astype(kind)


def gaussian_with(rng, shape, deviation, reach, cuts, heavy, kind=jnp.bfloat16):
    result = deviation * jax.random.normal(rng, shape, jnp.float32)
    if cuts:
        result = result * block_levels(rng, shape, cuts, -0.22, 0.18)
    return jnp.clip(with_spikes(result, jax.random.fold_in(rng, 3), *heavy), -reach, reach).astype(kind)


def setup_inputs(seed: int = 0) -> dict:
    keys = jax.random.split(jax.random.key(seed), 7)
    states = gaussian_with(keys[0], (B, S, D), 1.0, 16.0, ((0, 64),), (0, 2, 64, 4.0))
    hist_len = set_ends(jax.random.randint(keys[1], (B,), 1, ITEMS + 1), jax.random.fold_in(keys[1], 1), 1, ITEMS).astype(jnp.int32)
    norm_gain = jnp.clip(1.0 + 0.1 * jax.random.normal(keys[2], (D,), jnp.float32), 0.5, 1.5)
    qkv_weight = draw_qkv_weight(jax.random.fold_in(keys[6], 71), 0)
    output_weight = gaussian(keys[4], (H, DH, D), (H * DH) ** -0.5, 0.21875, ((0, 4),))
    cotangent = gaussian_with(keys[5], (B, S, D), 1.0, 16.0, ((0, 64),), (0, 2, 64, 4.0))
    return {"states": states, "hist_len": hist_len, "norm_gain": norm_gain, "qkv_weight": qkv_weight, "output_weight": output_weight, "cotangent": cotangent}


def reference(states, hist_len, norm_gain, qkv_weight, output_weight, cotangent):
    wide_states = states.astype(jnp.float32)
    inv_rms = lax.rsqrt(lax.optimization_barrier(jnp.mean(wide_states * wide_states, axis=-1, keepdims=True)) + 1e-06)
    unit = wide_states * inv_rms
    normed = (unit * norm_gain).astype(jnp.bfloat16)
    proj = jnp.einsum('bsd,dchk->bschk', normed.astype(jnp.float32), qkv_weight.astype(jnp.float32)).astype(jnp.bfloat16)
    queries = proj[:, :, 0].astype(jnp.float32)
    key_rows = proj[:, :, 1].astype(jnp.float32)
    value_rows = proj[:, :, 2].astype(jnp.float32)
    positions = jnp.arange(states.shape[1], dtype=jnp.int32)
    keep_mask = positions[None, :] < LEVELS * hist_len[:, None]
    scores = jnp.einsum('bqhk,bphk->bhqp', queries, key_rows)
    masked = jnp.where(keep_mask[:, None, None, :], scores, -1e+30)
    row_top = lax.optimization_barrier(jnp.max(masked, axis=-1, keepdims=True))
    exp_scores = jnp.exp(masked - row_top)
    attn_prob = exp_scores / lax.optimization_barrier(jnp.sum(exp_scores, axis=-1, keepdims=True))
    prob_bf = attn_prob.astype(jnp.bfloat16).astype(jnp.float32)
    attended_context = jnp.einsum('bhqp,bphk->bqhk', prob_bf, value_rows).astype(jnp.bfloat16)
    mixed_total_sum = jnp.einsum('zagm,gms->zas', attended_context.astype(jnp.float32), output_weight.astype(jnp.float32))
    attended = (wide_states + mixed_total_sum).astype(jnp.bfloat16)
    masked_cotangent = jnp.where(keep_mask[:, :, None], cotangent, jnp.zeros_like(cotangent)).astype(jnp.float32)
    output_weight_gradient = jnp.einsum('wmep,wmx->epx', attended_context.astype(jnp.float32), masked_cotangent)
    context_gradient = jnp.einsum('uxy,wgy->uxwg', masked_cotangent, output_weight.astype(jnp.float32)).astype(jnp.bfloat16).astype(jnp.float32)
    grad_prob = jnp.einsum('bqhk,bphk->bhqp', context_gradient, value_rows)
    row_delta = lax.optimization_barrier(jnp.sum(attn_prob * grad_prob, axis=-1, keepdims=True))
    grad_score = (attn_prob * (grad_prob - row_delta)).astype(jnp.bfloat16).astype(jnp.float32)
    grad_query = jnp.einsum('bhqp,bphk->bqhk', grad_score, key_rows)
    grad_key = jnp.einsum('bhqp,bqhk->bphk', grad_score, queries)
    grad_value = jnp.einsum('bhqp,bqhk->bphk', prob_bf, context_gradient)
    grad_proj = jnp.stack([grad_query, grad_key, grad_value], axis=2).astype(jnp.bfloat16).astype(jnp.float32)
    grad_qkv = jnp.einsum('bsd,bschk->dchk', normed.astype(jnp.float32), grad_proj)
    grad_normed = jnp.einsum('bschk,dchk->bsd', grad_proj, qkv_weight.astype(jnp.float32))
    grad_gain = lax.optimization_barrier(jnp.sum(grad_normed * unit, axis=(0, 1)))
    grad_unit = grad_normed * norm_gain
    row_corr = lax.optimization_barrier(jnp.mean(grad_unit * unit, axis=-1, keepdims=True))
    grad_states = (masked_cotangent + inv_rms * (grad_unit - unit * row_corr)).astype(jnp.bfloat16)
    return (attended, grad_states, grad_qkv, output_weight_gradient, grad_gain)
```

```python
import jax, jax.numpy as jnp
from jax import lax
from jax.experimental import pallas as pl
from jax.experimental.pallas import tpu as pltpu
from jax.sharding import PartitionSpec as P

S=80; D=768; NB=4; R=NB*S
f32=jnp.float32; bf16=jnp.bfloat16

def nt(a,b): return lax.dot_general(a,b,(((1,),(1,)),((),())),preferred_element_type=f32)
def nn(a,b): return lax.dot_general(a,b,(((1,),(0,)),((),())),preferred_element_type=f32)
def tn(a,b): return lax.dot_general(a,b,(((0,),(0,)),((),())),preferred_element_type=f32)

def attend(q,k,v,dc,keys):
    lane=lax.broadcasted_iota(jnp.int32,(1,256),1)//64
    ms=[(lane==h).astype(bf16) for h in range(3)]
    mf=[m.astype(f32) for m in ms]
    z=jnp.zeros((16,256),bf16)
    qs=jnp.concatenate([q*m for m in ms]+[z],axis=0)
    dst=jnp.concatenate([dc*m for m in ms]+[z],axis=0)
    st=nt(k,qs)
    keep=lax.broadcasted_iota(jnp.int32,(S,256),0)<keys
    st=jnp.where(keep,st,-1e30)
    e=jnp.exp(st-jnp.max(st,axis=0,keepdims=True))
    p=e*(1.0/jnp.sum(e,axis=0,keepdims=True))
    pb=p.astype(bf16)
    o=tn(pb,v)
    ctx=o[0:S]*mf[0]+o[S:2*S]*mf[1]+o[2*S:3*S]*mf[2]
    dp=nt(v,dst)
    ds=(p*(dp-jnp.sum(p*dp,axis=0,keepdims=True))).astype(bf16)
    dv=nn(pb,dst)
    dk=nn(ds,qs)
    u=tn(ds,k)
    dq=u[0:S]*mf[0]+u[S:2*S]*mf[1]+u[2*S:3*S]*mf[2]
    return ctx.astype(bf16), dq.astype(bf16), dk.astype(bf16), dv.astype(bf16)

def prologue(states,cot,hist,gain,normed,mcot,inv):
    def body(b,_):
        r=pl.ds(pl.multiple_of(b*S,S),S)
        x=states[r,:].astype(f32)
        iv=lax.rsqrt(jnp.mean(x*x,axis=-1,keepdims=True)+1e-6)
        inv[r,:]=jnp.broadcast_to(iv,(S,128))
        normed[r,:]=((x*iv)*gain[...]).astype(bf16)
        keep=lax.broadcasted_iota(jnp.int32,(S,D),0)<4*hist[b]
        mcot[r,:]=jnp.where(keep,cot[r,:].astype(f32),0.0).astype(bf16)
        return 0
    lax.fori_loop(0,16,body,0)

def block(slot,i,first,hist,wq,wo,normed,mcot,proj,dctx,ctx,gproj,att,gn):
    r0=pl.multiple_of(i*R,R)
    rows=pl.ds(r0,R)
    proj[...]=nt(normed[rows,:],wq[slot]).astype(bf16)
    dctx[...]=nt(mcot[rows,:],wo[slot]).astype(bf16)
    for j in range(NB):
        a=slice(j*S,(j+1)*S)
        c,dq,dk,dv=attend(proj[a,0:256],proj[a,256:512],proj[a,512:768],dctx[a,:],4*hist[i*NB+j])
        rr=pl.ds(pl.multiple_of(r0+j*S,S),S)
        ctx[rr,:]=c
        gproj[rr,0:256]=dq
        gproj[rr,256:512]=dk
        gproj[rr,512:768]=dv
    t=nn(ctx[rows,:],wo[slot])
    att[rows,:]=t if first else att[rows,:]+t
    t=nn(gproj[rows,:],wq[slot])
    gn[rows,:]=t if first else gn[rows,:]+t

def wgrads(normed,mcot,ctx,gproj,g):
    def body(t,_):
        c=pl.ds(pl.multiple_of(t*256,256),256)
        g[c,0:768]=tn(normed[:,c],gproj[...]).astype(g.dtype)
        g[c,768:1024]=tn(mcot[:,c],ctx[...]).astype(g.dtype)
        return 0
    lax.fori_loop(0,3,body,0)

def epilogue(states,gain,mcot,inv,att,gn,attended,gstates,gg):
    gg[...]=jnp.zeros_like(gg)
    def body(b,_):
        r=pl.ds(pl.multiple_of(b*S,S),S)
        x=states[r,:].astype(f32)
        iv=inv[r,0:1]
        attended[r,:]=(x+att[r,:]).astype(bf16)
        u=x*iv
        n=gn[r,:]
        gg[...]+=jnp.sum(n*u,axis=0,keepdims=True)
        gu=n*gain[...]
        m=jnp.mean(gu*u,axis=-1,keepdims=True)
        gstates[r,:]=(mcot[r,:].astype(f32)+iv*(gu-u*m)).astype(bf16)
        return 0
    lax.fori_loop(0,16,body,0)

def kernel(hist,states,cot,gain,wq,wo,attended,gstates,g,gg,normed,mcot,inv,proj,dctx,ctx,gproj,att,gn):
    prologue(states,cot,hist,gain,normed,mcot,inv)
    def b0(i,_):
        block(0,i,True,hist,wq,wo,normed,mcot,proj,dctx,ctx,gproj,att,gn); return 0
    lax.fori_loop(0,16//NB,b0,0)
    wgrads(normed,mcot,ctx,gproj,g)
    def b1(t,_):
        block(1+t//(16//NB),lax.rem(t,16//NB),False,hist,wq,wo,normed,mcot,proj,dctx,ctx,gproj,att,gn); return 0
    lax.fori_loop(0,3*(16//NB),b1,0)
    epilogue(states,gain,mcot,inv,att,gn,attended,gstates,gg)

V=pl.BlockSpec(memory_space=pltpu.VMEM)
def compute(hist,states,cot,gain,wq,wo):
    n=16*S
    return pl.pallas_call(kernel,
        out_shape=(jax.ShapeDtypeStruct((n,D),bf16),jax.ShapeDtypeStruct((n,D),bf16),jax.ShapeDtypeStruct((D,1024),f32),jax.ShapeDtypeStruct((1,D),f32)),
        in_specs=[pl.BlockSpec(memory_space=pltpu.SMEM)]+[V]*5, out_specs=(V,)*4,
        scratch_shapes=[pltpu.VMEM((n,D),bf16),pltpu.VMEM((n,D),bf16),pltpu.VMEM((n,128),f32),
            pltpu.VMEM((R,D),bf16),pltpu.VMEM((R,256),bf16),pltpu.VMEM((n,256),bf16),pltpu.VMEM((n,D),bf16),
            pltpu.VMEM((n,D),f32),pltpu.VMEM((n,D),f32)],
        compiler_params=pltpu.CompilerParams(vmem_limit_bytes=60*2**20),
    )(hist,states,cot,gain,wq,wo)


def summed(x, axis):
    n = lax.axis_size(axis)
    y = lax.all_to_all(x.reshape(n, x.shape[0] // n, x.shape[1]), axis, 0, 0, tiled=True)
    return jnp.sum(y.astype(f32), axis=0)


def body(states, hist_len, norm_gain, qkv_weight, output_weight, cotangent):
    me = lax.axis_index("mp")
    order = lax.rem(me + jnp.arange(4), 4)
    wq = jnp.transpose(qkv_weight, (1, 2, 3, 0))
    wq = lax.all_gather(wq, "mp")[order]
    wo = lax.all_gather(output_weight, "mp")[order]
    wq = jnp.pad(wq, ((0, 0), (0, 0), (0, 1), (0, 0), (0, 0))).reshape(4, 768, 768)
    wo = jnp.pad(wo, ((0, 0), (0, 1), (0, 0), (0, 0))).reshape(4, 256, 768)
    attended, gstates, g, gg = compute(
        hist_len, states.reshape(-1, D), cotangent.reshape(-1, D), norm_gain[None], wq, wo
    )
    g = g.reshape(768, 4, 4, 64)[:, :, :3].reshape(768, 768).astype(bf16)
    g = summed(g, "dp").reshape(12, 4, 3, 64)
    gg = summed(jnp.reshape(gg, (768, 1)).astype(bf16), "dp").reshape(12)
    shape = states.shape
    return (
        attended.reshape(shape),
        gstates.reshape(shape),
        g[:, :3],
        jnp.transpose(g[:, 3], (1, 2, 0)),
        gg,
    )


def solution(mesh):
    placed = (
        P("dp", None, None),
        P("dp"),
        P(),
        P(None, None, "mp", None),
        P("mp", None, None),
        P("dp", None, None),
    )
    return jax.shard_map(
        body,
        mesh=mesh,
        in_specs=placed,
        out_specs=(
            P("dp", None, None),
            P("dp", None, None),
            P("dp", None, "mp", None),
            P("mp", None, "dp"),
            P("dp"),
        ),
        check_vma=False,
    )
```

```python
import jax, jax.numpy as jnp
from jax import lax
from jax.experimental import pallas as pl
from jax.experimental.pallas import tpu as pltpu
from jax.sharding import PartitionSpec as P

S=80; D=768; NB=4; R=NB*S
f32=jnp.float32; bf16=jnp.bfloat16

def nt(a,b): return lax.dot_general(a,b,(((1,),(1,)),((),())),preferred_element_type=f32)
def nn(a,b): return lax.dot_general(a,b,(((1,),(0,)),((),())),preferred_element_type=f32)
def tn(a,b): return lax.dot_general(a,b,(((0,),(0,)),((),())),preferred_element_type=f32)

def attend(q,k,v,dc,keys):
    lane=lax.broadcasted_iota(jnp.int32,(1,256),1)//64
    ms=[(lane==h).astype(bf16) for h in range(3)]
    mf=[m.astype(f32) for m in ms]
    z=jnp.zeros((16,256),bf16)
    qs=jnp.concatenate([q*m for m in ms]+[z],axis=0)
    dst=jnp.concatenate([dc*m for m in ms]+[z],axis=0)
    st=nt(k,qs)
    keep=lax.broadcasted_iota(jnp.int32,(S,256),0)<keys
    st=jnp.where(keep,st,-1e30)
    e=jnp.exp(st-jnp.max(st,axis=0,keepdims=True))
    p=e*(1.0/jnp.sum(e,axis=0,keepdims=True))
    pb=p.astype(bf16)
    o=tn(pb,v)
    ctx=o[0:S]*mf[0]+o[S:2*S]*mf[1]+o[2*S:3*S]*mf[2]
    dp=nt(v,dst)
    ds=(p*(dp-jnp.sum(p*dp,axis=0,keepdims=True))).astype(bf16)
    dv=nn(pb,dst)
    dk=nn(ds,qs)
    u=tn(ds,k)
    dq=u[0:S]*mf[0]+u[S:2*S]*mf[1]+u[2*S:3*S]*mf[2]
    return ctx.astype(bf16), dq.astype(bf16), dk.astype(bf16), dv.astype(bf16)

def prologue(states,cot,hist,gain,normed,mcot,inv):
    def body(b,_):
        r=pl.ds(pl.multiple_of(b*S,S),S)
        x=states[r,:].astype(f32)
        iv=lax.rsqrt(jnp.mean(x*x,axis=-1,keepdims=True)+1e-6)
        inv[r,:]=jnp.broadcast_to(iv,(S,128))
        normed[r,:]=((x*iv)*gain[...]).astype(bf16)
        keep=lax.broadcasted_iota(jnp.int32,(S,D),0)<4*hist[b]
        mcot[r,:]=jnp.where(keep,cot[r,:].astype(f32),0.0).astype(bf16)
        return 0
    lax.fori_loop(0,16,body,0)

MESH = pl.DeviceIdType.MESH


def block(slot, i, hist, w, normed, mcot, proj, dctx, ctx, gproj, att, gn):
    r0 = pl.multiple_of(i * R, R)
    rows = pl.ds(r0, R)
    proj[...] = nt(normed[rows, :], w[slot, 0:3].reshape(768, D)).astype(bf16)
    dctx[...] = nt(mcot[rows, :], w[slot, 3]).astype(bf16)
    for j in range(NB):
        a = slice(j * S, (j + 1) * S)
        c, dq, dk, dv = attend(
            proj[a, 0:256], proj[a, 256:512], proj[a, 512:768], dctx[a, :], 4 * hist[i * NB + j]
        )
        rr = pl.ds(pl.multiple_of(r0 + j * S, S), S)
        ctx[rr, :] = c
        gproj[rr, 0:256] = dq
        gproj[rr, 256:512] = dk
        gproj[rr, 512:768] = dv
    att[rows, :] += nn(ctx[rows, :], w[slot, 3])
    gn[rows, :] += nn(gproj[rows, :], w[slot, 0:3].reshape(768, D))


def wgrads(normed, mcot, ctx, gproj, gs):
    def body(t, _):
        c = pl.ds(pl.multiple_of(t * 256, 256), 256)
        g = tn(normed[:, c], gproj[...])
        o = tn(mcot[:, c], ctx[...])
        gs[0, c, 0:128] = g[:, 0:128].astype(bf16)
        gs[0, c, 128:256] = g[:, 256:384].astype(bf16)
        gs[0, c, 256:384] = g[:, 512:640].astype(bf16)
        gs[1, c, 0:128] = o[:, 0:128].astype(bf16)
        gs[1, c, 128:256] = (g[:, 128:256] + pltpu.roll(g[:, 384:512], 64, 1)).astype(bf16)
        gs[1, c, 256:384] = (g[:, 640:768] + pltpu.roll(o[:, 128:256], 64, 1)).astype(bf16)
        return 0

    lax.fori_loop(0, 3, body, 0)


def local_gain(states, inv, gn, gg):
    gg[...] = jnp.zeros_like(gg)

    def body(b, _):
        r = pl.ds(pl.multiple_of(b * S, S), S)
        t = gn[r, :] * (states[r, :].astype(f32) * inv[r, 0:1])
        gg[...] += jnp.sum(t.reshape(S // 8, 8, D), axis=0)
        return 0

    lax.fori_loop(0, 16, body, 0)


def epilogue(states, gain, mcot, inv, att, gn, attended, gstates):
    def body(b, _):
        r = pl.ds(pl.multiple_of(b * S, S), S)
        x = states[r, :].astype(f32)
        iv = inv[r, 0:1]
        attended[r, :] = (x + att[r, :]).astype(bf16)
        u = x * iv
        gu = gn[r, :] * gain[...]
        m = jnp.mean(gu * u, axis=-1, keepdims=True)
        gstates[r, :] = (mcot[r, :].astype(f32) + iv * (gu - u * m)).astype(bf16)
        return 0

    lax.fori_loop(0, 16, body, 0)


def kernel(
    hist, states, cot, gain, wq_hbm, wo_hbm,
    attended, gstates, gq_out, go_out, gg_out,
    w, normed, mcot, inv, proj, dctx, ctx, gproj, att, gn,
    gs, ra, sb, rb, sc, rc, sd, rd, fin, gg, gb,
    load_sem, send_sem, recv_sem,
):
    dp, zl = lax.axis_index("dp"), lax.axis_index("mp")
    x, y, zh, core = dp // 16, lax.rem(dp // 4, 4), lax.rem(dp // 2, 2), lax.rem(dp, 2)
    z = zh * 4 + zl

    def dev(x, y, z, core):
        return (((x * 4 + y) * 2 + z // 4) * 2 + core, lax.rem(z, 4))

    def at_z(k):
        return dev(x, y, lax.rem(z + k, 8), core)

    up, down, up2, down2, far = at_z(1), at_z(7), at_z(2), at_z(6), at_z(4)
    twin = dev(x, y, z, 1 - core)
    xs = [dev(lax.rem(x + k, 4), y, z, core) for k in (1, 2, 3)]
    ys = [dev(x, lax.rem(y + k, 4), z, core) for k in (1, 2, 3)]

    loads = [
        pltpu.make_async_copy(wq_hbm, w.at[0, pl.ds(0, 3), pl.ds(0, 192), :], load_sem.at[0]),
        pltpu.make_async_copy(wo_hbm, w.at[0, 3, pl.ds(0, 192), :], load_sem.at[1]),
    ]
    for c in loads:
        c.start()
    barrier = pltpu.get_barrier_semaphore()
    peers = [up, down, up2, down2, far, twin] + xs + ys
    for p in peers:
        pl.semaphore_signal(barrier, inc=1, device_id=p, device_id_type=MESH)

    count = [0]

    def remote(src, dst, device):
        k = count[0]
        count[0] += 1
        return pltpu.make_async_remote_copy(
            src_ref=src, dst_ref=dst, send_sem=send_sem.at[k], recv_sem=recv_sem.at[k],
            device_id=device, device_id_type=MESH,
        )

    def part(slot, first, n):
        return w.at[slot, pl.ds(first, n), pl.ds(0, 192), :]

    c2 = 2 * core
    to_up = remote(part(0, c2, 2), part(1, c2, 2), up)
    to_down = remote(part(0, c2, 2), part(2, c2, 2), down)
    to_up2 = remote(part(0, c2, 1), part(3, c2, 1), up2)
    to_down2 = remote(part(0, c2 + 1, 1), part(3, c2 + 1, 1), down2)
    pass_on = [remote(part(s, c2, 2), part(s, c2, 2), twin) for s in (1, 2, 3)]
    st_a = [remote(gs.at[1 - core], ra, twin), remote(gg.at[0], gb.at[0], twin)]
    st_b, st_c = [], []
    for k in (1, 2, 3):
        chunk = pl.ds(pl.multiple_of(lax.rem(x + k, 4) * 192, 192), 192)
        st_b.append(remote(sb.at[chunk, :], rb.at[k - 1], xs[k - 1]))
        st_b.append(remote(gg.at[1], gb.at[k], xs[k - 1]))
    for k in (1, 2, 3):
        chunk = pl.ds(pl.multiple_of(lax.rem(y + k, 4) * 48, 48), 48)
        st_c.append(remote(sc.at[chunk, :], rc.at[k - 1], ys[k - 1]))
        st_c.append(remote(gg.at[2], gb.at[3 + k], ys[k - 1]))
    st_d = [remote(sd.at[0], rd, far), remote(gg.at[3], gb.at[7], far)]
    st_e = [remote(sd.at[1], fin.at[core], twin)]
    st_e += [remote(gg.at[4], gb.at[8 + k], d) for k, d in enumerate((up, down, up2))]

    def start(cs):
        for c in cs:
            c.start()

    def wait(cs):
        for c in cs:
            c.wait()

    for s in range(4):
        for p in range(4):
            w[s, p, 192:256, :] = jnp.zeros((64, D), bf16)
    att[...] = jnp.zeros_like(att)
    gn[...] = jnp.zeros_like(gn)
    for c in loads:
        c.wait()
    pl.semaphore_wait(barrier, len(peers))
    start([to_up, to_down, to_up2, to_down2])
    prologue(states, cot, hist, gain, normed, mcot, inv)

    def step(t, _):
        slot = t // (16 // NB)
        i = lax.rem(t, 16 // NB)

        @pl.when(t == 4)
        def _():
            pass_on[0].wait()

        @pl.when(t == 8)
        def _():
            pass_on[1].wait()

        @pl.when(t == 12)
        def _():
            pass_on[2].wait()

        block(slot, i, hist, w, normed, mcot, proj, dctx, ctx, gproj, att, gn)

        @pl.when(t == 3)
        def _():
            to_up.wait()
            pass_on[0].start()
            to_down.wait()
            pass_on[1].start()
            wgrads(normed, mcot, ctx, gproj, gs)
            local_gain(states, inv, gn, gg.at[0])
            start(st_a)

        @pl.when(t == 4)
        def _():
            wait(st_a)
            sb[...] = (gs[core].astype(f32) + ra[...].astype(f32)).astype(bf16)
            gg[1] = gg[0] + gb[0]

        @pl.when(t == 5)
        def _():
            start(st_b)

        @pl.when(t == 7)
        def _():
            to_up2.wait()
            to_down2.wait()
            pass_on[2].start()
            wait(st_b)
            own = sb[pl.ds(pl.multiple_of(x * 192, 192), 192), :].astype(f32)
            for k in range(3):
                own += rb[k].astype(f32)
            sc[...] = own.astype(bf16)
            gg[2] = gg[1] + (gb[1] + gb[2] + gb[3])

        @pl.when(t == 8)
        def _():
            start(st_c)

        @pl.when(t == 9)
        def _():
            wait(st_c)
            own = sc[pl.ds(pl.multiple_of(y * 48, 48), 48), :].astype(f32)
            for k in range(3):
                own += rc[k].astype(f32)
            sd[0] = own.astype(bf16)
            gg[3] = gg[2] + (gb[4] + gb[5] + gb[6])

        @pl.when(t == 10)
        def _():
            start(st_d)

        @pl.when(t == 11)
        def _():
            wait(st_d)
            both = (sd[0].astype(f32) + rd[...].astype(f32)).astype(bf16)
            sd[1] = both
            fin[core] = both
            gg[4] = gg[3] + gb[7]

        @pl.when(t == 12)
        def _():
            start(st_e)

        @pl.when(t == 13)
        def _():
            wait(st_e)
            total = gg[4] + (gb[8] + gb[9] + gb[10])
            total = jnp.sum(total, axis=0, keepdims=True)
            total = jnp.broadcast_to(total, (8, D))
            gg_out[...] = pltpu.roll(total, lax.rem(D - 12 * dp, D), 1)[0:1, 0:12]
            mine = 12 * (2 * zh + core)
            pad = jnp.zeros((80, 384), f32)
            for h in range(2):
                rows = jnp.concatenate([fin[h].astype(f32), pad], axis=0).T
                cols = pltpu.roll(rows, lax.rem(128 - mine, 128), 1)[:, 0:12]
                if h == 0:
                    for c in range(3):
                        gq_out[192 * c : 192 * c + 128, :] = cols[128 * c : 128 * c + 128]
                else:
                    go_out[0:128, :] = cols[0:128]
                    for c in range(3):
                        gq_out[192 * c + 128 : 192 * c + 192, :] = cols[128 + 64 * c : 192 + 64 * c]
                    go_out[128:192, :] = cols[320:384]

        return 0

    lax.fori_loop(0, 64 // NB, step, 0)
    epilogue(states, gain, mcot, inv, att, gn, attended, gstates)


VMEM = pl.BlockSpec(memory_space=pltpu.VMEM)
ANY = pl.BlockSpec(memory_space=pl.ANY)
COPIES = 29


def compute(hist, states, cot, gain, wq, wo):
    n = 16 * S
    return pl.pallas_call(
        kernel,
        out_shape=(
            jax.ShapeDtypeStruct((n, D), bf16),
            jax.ShapeDtypeStruct((n, D), bf16),
            jax.ShapeDtypeStruct((576, 12), f32),
            jax.ShapeDtypeStruct((192, 12), f32),
            jax.ShapeDtypeStruct((1, 12), f32),
        ),
        in_specs=[pl.BlockSpec(memory_space=pltpu.SMEM), VMEM, VMEM, VMEM, ANY, ANY],
        out_specs=(VMEM,) * 5,
        scratch_shapes=[
            pltpu.VMEM((4, 4, 256, D), bf16),
            pltpu.VMEM((n, D), bf16),
            pltpu.VMEM((n, D), bf16),
            pltpu.VMEM((n, 128), f32),
            pltpu.VMEM((R, D), bf16),
            pltpu.VMEM((R, 256), bf16),
            pltpu.VMEM((n, 256), bf16),
            pltpu.VMEM((n, D), bf16),
            pltpu.VMEM((n, D), f32),
            pltpu.VMEM((n, D), f32),
            pltpu.VMEM((2, D, 384), bf16),
            pltpu.VMEM((D, 384), bf16),
            pltpu.VMEM((D, 384), bf16),
            pltpu.VMEM((3, 192, 384), bf16),
            pltpu.VMEM((192, 384), bf16),
            pltpu.VMEM((3, 48, 384), bf16),
            pltpu.VMEM((2, 48, 384), bf16),
            pltpu.VMEM((48, 384), bf16),
            pltpu.VMEM((2, 48, 384), bf16),
            pltpu.VMEM((5, 8, D), f32),
            pltpu.VMEM((11, 8, D), f32),
            pltpu.SemaphoreType.DMA((2,)),
            pltpu.SemaphoreType.DMA((COPIES,)),
            pltpu.SemaphoreType.DMA((COPIES,)),
        ],
        compiler_params=pltpu.CompilerParams(
            vmem_limit_bytes=60 * 2**20, collective_id=0, has_side_effects=True
        ),
    )(hist, states, cot, gain, wq, wo)


def body(states, hist_len, norm_gain, qkv_weight, output_weight, cotangent):
    wq = jnp.transpose(qkv_weight, (1, 2, 3, 0)).reshape(3, 192, D)
    wo = output_weight.reshape(192, D)
    attended, gstates, gq, go, gg = compute(
        hist_len, states.reshape(-1, D), cotangent.reshape(-1, D), norm_gain[None], wq, wo
    )
    shape = states.shape
    return (
        attended.reshape(shape),
        gstates.reshape(shape),
        jnp.transpose(gq.reshape(3, 3, 64, 12), (3, 0, 1, 2)),
        go.reshape(3, 64, 12),
        gg.reshape(12),
    )


def solution(mesh):
    placed = (
        P("dp", None, None),
        P("dp"),
        P(),
        P(None, None, "mp", None),
        P("mp", None, None),
        P("dp", None, None),
    )
    return jax.shard_map(
        body,
        mesh=mesh,
        in_specs=placed,
        out_specs=(
            P("dp", None, None),
            P("dp", None, None),
            P("dp", None, "mp", None),
            P("mp", None, "dp"),
            P("dp"),
        ),
        check_vma=False,
    )
```

```python
import jax, jax.numpy as jnp
from jax import lax
from jax.experimental import pallas as pl
from jax.experimental.pallas import tpu as pltpu
from jax.sharding import PartitionSpec as P

S=80; D=768; NB=4; R=NB*S; PER=16//NB
f32=jnp.float32; bf16=jnp.bfloat16

def nt(a,b): return lax.dot_general(a,b,(((1,),(1,)),((),())),preferred_element_type=f32)
def nn(a,b): return lax.dot_general(a,b,(((1,),(0,)),((),())),preferred_element_type=f32)
def tn(a,b): return lax.dot_general(a,b,(((0,),(0,)),((),())),preferred_element_type=f32)

def prologue(states,cot,hist,gain,normed,mcot,inv):
    def body(b,_):
        r=pl.ds(pl.multiple_of(b*S,S),S)
        x=states[r,:].astype(f32)
        iv=lax.rsqrt(jnp.mean(x*x,axis=-1,keepdims=True)+1e-6)
        inv[r,:]=jnp.broadcast_to(iv,(S,128))
        normed[r,:]=((x*iv)*gain).astype(bf16)
        keep=lax.broadcasted_iota(jnp.int32,(S,D),0)<4*hist[b]
        mcot[r,:]=jnp.where(keep,cot[r,:].astype(f32),0.0).astype(bf16)
        return 0
    lax.fori_loop(0,16,body,0)

MESH = pl.DeviceIdType.MESH


def fill(t, w, normed, mcot, kb, vb, qs, dcs):
    slot = jnp.minimum(t // (PER), 3)
    buf = lax.rem(t, 2)
    rows = pl.ds(pl.multiple_of(lax.rem(t, PER) * R, R), R)
    low = lax.broadcasted_iota(jnp.int32, (S, 128), 1) < 64
    pr = nt(normed[rows, :], w[slot, 0:3].reshape(768, D))
    dc = nt(mcot[rows, :], w[slot, 3])

    def stack(ref, j, v):
        lo = v[:, 0:128]
        ref[buf, j, 0:S, 0:128] = jnp.where(low, lo, 0.0).astype(bf16)
        ref[buf, j, S : 2 * S, 0:128] = jnp.where(low, 0.0, lo).astype(bf16)
        ref[buf, j, 2 * S : 3 * S, 128:256] = v[:, 128:256].astype(bf16)

    for j in range(NB):
        a = slice(j * S, (j + 1) * S)
        stack(qs, j, pr[a, 0:256])
        kb[buf, j] = pr[a, 256:512].astype(bf16)
        vb[buf, j] = pr[a, 512:768].astype(bf16)
        stack(dcs, j, dc[a])


def push(t, w, ctx, gproj, att, gn):
    slot = t // (PER)
    rows = pl.ds(pl.multiple_of(lax.rem(t, PER) * R, R), R)
    att[rows, :] += nn(ctx[rows, :], w[slot, 3])
    gn[rows, :] += nn(gproj[rows, :], w[slot, 0:3].reshape(768, D))


def attend(t, hist, w, kb, vb, qs, dcs, ctx, gproj, att, gn):
    buf = lax.rem(t, 2)
    i = lax.rem(t, PER)
    row = lax.broadcasted_iota(jnp.int32, (S, 256), 0)
    low = lax.broadcasted_iota(jnp.int32, (S, 128), 1) < 64
    st = [nt(kb[buf, j], qs[buf, j]) for j in range(NB)]
    dp = [nt(vb[buf, j], dcs[buf, j]) for j in range(NB)]
    push(t - 1 + jnp.where(t == 0, PER, 0), w, ctx, gproj, att, gn)
    pb, ds = [], []
    for j in range(NB):
        x = jnp.where(row < 4 * hist[i * NB + j], st[j], -1e30)
        e = jnp.exp(x - jnp.max(x, axis=0, keepdims=True))
        p = e * (1.0 / jnp.sum(e, axis=0, keepdims=True))
        pb.append(p.astype(bf16))
        pd = p * dp[j]
        ds.append((pd - p * jnp.sum(pd, axis=0, keepdims=True)).astype(bf16))

    def heads(o):
        return jnp.where(low, o[0:S, 0:128], o[S : 2 * S, 0:128]).astype(bf16), o[
            2 * S : 3 * S, 128:256
        ].astype(bf16)

    for j in range(NB):
        rr = pl.ds(pl.multiple_of((i * NB + j) * S, S), S)
        ctx[rr, 0:128], ctx[rr, 128:256] = heads(tn(pb[j], vb[buf, j]))
        gproj[rr, 0:128], gproj[rr, 128:256] = heads(tn(ds[j], kb[buf, j]))
        gproj[rr, 256:512] = nn(ds[j], qs[buf, j]).astype(bf16)
        gproj[rr, 512:768] = nn(pb[j], dcs[buf, j]).astype(bf16)


def wgrads(normed, mcot, ctx, gproj, gs):
    def body(t, _):
        c = pl.ds(pl.multiple_of(t * 256, 256), 256)
        g = tn(normed[:, c], gproj[...])
        o = tn(mcot[:, c], ctx[...])
        gs[0, c, 0:128] = g[:, 0:128].astype(bf16)
        gs[0, c, 128:256] = g[:, 256:384].astype(bf16)
        gs[0, c, 256:384] = g[:, 512:640].astype(bf16)
        gs[1, c, 0:128] = o[:, 0:128].astype(bf16)
        gs[1, c, 128:256] = (g[:, 128:256] + pltpu.roll(g[:, 384:512], 64, 1)).astype(bf16)
        gs[1, c, 256:384] = (g[:, 640:768] + pltpu.roll(o[:, 128:256], 64, 1)).astype(bf16)
        return 0

    lax.fori_loop(0, 3, body, 0)


def local_gain(states, inv, gn, gg):
    gg[...] = jnp.zeros_like(gg)

    def body(b, _):
        r = pl.ds(pl.multiple_of(b * S, S), S)
        t = gn[r, :] * (states[r, :].astype(f32) * inv[r, 0:1])
        gg[...] += jnp.sum(t.reshape(S // 8, 8, D), axis=0)
        return 0

    lax.fori_loop(0, 16, body, 0)


def epilogue(states, gain, mcot, inv, att, gn, attended, gstates):
    def body(b, _):
        r = pl.ds(pl.multiple_of(b * S, S), S)
        x = states[r, :].astype(f32)
        iv = inv[r, 0:1]
        attended[r, :] = (x + att[r, :]).astype(bf16)
        u = x * iv
        gu = gn[r, :] * gain
        m = jnp.mean(gu * u, axis=-1, keepdims=True)
        gstates[r, :] = (mcot[r, :].astype(f32) + iv * (gu - u * m)).astype(bf16)
        return 0

    lax.fori_loop(0, 16, body, 0)


def kernel(
    hist, states_hbm, cot_hbm, gain_hbm, wq_hbm, wo_hbm,
    attended, gstates, gq_out, go_out, gg_out,
    states, cot, gain, w, normed, mcot, inv, kb, vb, qs, dcs, ctx, gproj, att, gn,
    gs, ra, sb, rb, sc, rc, sd, rd, fin, rows, gg, gb,
    load_sem, send_sem, recv_sem,
):
    dp, zl = lax.axis_index("dp"), lax.axis_index("mp")
    x, y, zh, core = dp // 16, lax.rem(dp // 4, 4), lax.rem(dp // 2, 2), lax.rem(dp, 2)
    z = zh * 4 + zl

    def dev(x, y, z, core):
        return (((x * 4 + y) * 2 + z // 4) * 2 + core, lax.rem(z, 4))

    def at_z(k):
        return dev(x, y, lax.rem(z + k, 8), core)

    up, down, up2, down2, far = at_z(1), at_z(7), at_z(2), at_z(6), at_z(4)
    twin = dev(x, y, z, 1 - core)
    xs = [dev(lax.rem(x + k, 4), y, z, core) for k in (1, 2, 3)]
    ys = [dev(x, lax.rem(y + k, 4), z, core) for k in (1, 2, 3)]

    loads = [
        pltpu.make_async_copy(wq_hbm, w.at[0, pl.ds(0, 3), pl.ds(0, 192), :], load_sem.at[0]),
        pltpu.make_async_copy(wo_hbm, w.at[0, 3, pl.ds(0, 192), :], load_sem.at[1]),
        pltpu.make_async_copy(gain_hbm, gain, load_sem.at[2]),
        pltpu.make_async_copy(states_hbm, states, load_sem.at[3]),
        pltpu.make_async_copy(cot_hbm, cot, load_sem.at[4]),
    ]
    for c in loads:
        c.start()
    barrier = pltpu.get_barrier_semaphore()
    peers = [up, down, up2, down2, far, twin] + xs + ys
    for p in peers:
        pl.semaphore_signal(barrier, inc=1, device_id=p, device_id_type=MESH)

    count = [0]

    def remote(src, dst, device):
        k = count[0]
        count[0] += 1
        return pltpu.make_async_remote_copy(
            src_ref=src, dst_ref=dst, send_sem=send_sem.at[k], recv_sem=recv_sem.at[k],
            device_id=device, device_id_type=MESH,
        )

    def part(slot, first, n):
        return w.at[slot, pl.ds(first, n), pl.ds(0, 192), :]

    c2 = 2 * core
    to_up = remote(part(0, c2, 2), part(1, c2, 2), up)
    to_down = remote(part(0, c2, 2), part(2, c2, 2), down)
    to_up2 = remote(part(0, c2, 1), part(3, c2, 1), up2)
    to_down2 = remote(part(0, c2 + 1, 1), part(3, c2 + 1, 1), down2)
    pass_on = [remote(part(s, c2, 2), part(s, c2, 2), twin) for s in (1, 2, 3)]
    st_a = [remote(gs.at[1 - core], ra, twin), remote(gg.at[0], gb.at[0], twin)]
    st_b, st_c = [], []
    for k in (1, 2, 3):
        chunk = pl.ds(pl.multiple_of(lax.rem(x + k, 4) * 192, 192), 192)
        st_b.append(remote(sb.at[chunk, :], rb.at[k - 1], xs[k - 1]))
        st_b.append(remote(gg.at[1], gb.at[k], xs[k - 1]))
    for k in (1, 2, 3):
        chunk = pl.ds(pl.multiple_of(lax.rem(y + k, 4) * 48, 48), 48)
        st_c.append(remote(sc.at[chunk, :], rc.at[k - 1], ys[k - 1]))
        st_c.append(remote(gg.at[2], gb.at[3 + k], ys[k - 1]))
    st_d = [remote(sd.at[0], rd, far), remote(gg.at[3], gb.at[7], far)]
    st_e = [remote(sd.at[1], fin.at[core], twin)]
    st_e += [remote(gg.at[4], gb.at[8 + k], d) for k, d in enumerate((up, down, up2))]

    def start(cs):
        for c in cs:
            c.start()

    def wait(cs):
        for c in cs:
            c.wait()

    for s in range(4):
        for p in range(4):
            w[s, p, 192:256, :] = jnp.zeros((64, D), bf16)
    for r in (qs, dcs, ctx, gproj, att, gn):
        r[...] = jnp.zeros_like(r)
    for c in loads[0:2]:
        c.wait()
    pl.semaphore_wait(barrier, len(peers))
    start([to_up, to_down, to_up2, to_down2])
    for c in loads[2:]:
        c.wait()
    gain = gain[...].reshape(1, D)
    prologue(states, cot, hist, gain, normed, mcot, inv)

    fill(0, w, normed, mcot, kb, vb, qs, dcs)

    def early(t, _):
        attend(t, hist, w, kb, vb, qs, dcs, ctx, gproj, att, gn)
        fill(t + 1, w, normed, mcot, kb, vb, qs, dcs)
        return 0

    lax.fori_loop(0, PER - 1, early, 0)
    attend(PER - 1, hist, w, kb, vb, qs, dcs, ctx, gproj, att, gn)
    wgrads(normed, mcot, ctx, gproj, gs)
    to_up.wait()
    pass_on[0].start()
    to_down.wait()
    pass_on[1].start()
    st_a[0].start()
    pass_on[0].wait()
    fill(PER, w, normed, mcot, kb, vb, qs, dcs)

    def step(t, _):
        @pl.when(t == 7)
        def _():
            pass_on[1].wait()

        @pl.when(t == 11)
        def _():
            pass_on[2].wait()

        attend(t, hist, w, kb, vb, qs, dcs, ctx, gproj, att, gn)
        fill(t + 1, w, normed, mcot, kb, vb, qs, dcs)

        @pl.when(t == 4)
        def _():
            local_gain(states, inv, gn, gg.at[0])

        @pl.when(t == 5)
        def _():
            st_a[1].start()
            st_a[0].wait()
            sb[...] = (gs[core].astype(f32) + ra[...].astype(f32)).astype(bf16)

        @pl.when(t == 6)
        def _():
            start(st_b[0::2])
            st_a[1].wait()
            gg[1] = gg[0] + gb[0]

        @pl.when(t == 7)
        def _():
            start(st_b[1::2])

        @pl.when(t == 8)
        def _():
            wait(st_b)
            own = sb[pl.ds(pl.multiple_of(x * 192, 192), 192), :].astype(f32)
            for k in range(3):
                own += rb[k].astype(f32)
            sc[...] = own.astype(bf16)
            gg[2] = gg[1] + (gb[1] + gb[2] + gb[3])

        @pl.when(t == 9)
        def _():
            start(st_c)
            to_up2.wait()
            to_down2.wait()
            pass_on[2].start()

        @pl.when(t == 10)
        def _():
            wait(st_c)
            own = sc[pl.ds(pl.multiple_of(y * 48, 48), 48), :].astype(f32)
            for k in range(3):
                own += rc[k].astype(f32)
            sd[0] = own.astype(bf16)
            gg[3] = gg[2] + (gb[4] + gb[5] + gb[6])

        @pl.when(t == 11)
        def _():
            start(st_d)

        @pl.when(t == 12)
        def _():
            wait(st_d)
            both = (sd[0].astype(f32) + rd[...].astype(f32)).astype(bf16)
            sd[1] = both
            fin[core] = both
            gg[4] = gg[3] + gb[7]

        @pl.when(t == 13)
        def _():
            start(st_e)

        @pl.when(t == 14)
        def _():
            wait(st_e)
            total = gg[4] + (gb[8] + gb[9] + gb[10])
            total = jnp.sum(total, axis=0, keepdims=True)
            total = jnp.broadcast_to(total, (8, D))
            gg_out[...] = pltpu.roll(total, lax.rem(D - 12 * dp, D), 1)[0:1, 0:12]
            for h in range(2):
                part_h = fin[h].astype(f32)
                for q in range(4):
                    rows[q, 0:12, 384 * h : 384 * h + 384] = part_h[12 * q : 12 * q + 12]
            mine = rows[2 * zh + core, 0:12, :]
            for r in range(12):
                one = mine[r : r + 1]
                for c in range(3):
                    at = 512 + 64 * c
                    gq_out[r, c, 0:1, :] = one[:, 128 * c : 128 * c + 64]
                    gq_out[r, c, 1:2, :] = one[:, 128 * c + 64 : 128 * c + 128]
                    gq_out[r, c, 2:3, :] = one[:, at : at + 64]
            go_out[0] = mine[:, 384:448]
            go_out[1] = mine[:, 448:512]
            go_out[2] = mine[:, 704:768]

        return 0

    lax.fori_loop(PER, 4 * PER - 1, step, 0)
    attend(4 * PER - 1, hist, w, kb, vb, qs, dcs, ctx, gproj, att, gn)
    push(4 * PER - 1, w, ctx, gproj, att, gn)
    epilogue(states, gain, mcot, inv, att, gn, attended, gstates)


VMEM = pl.BlockSpec(memory_space=pltpu.VMEM)
HBM = pl.BlockSpec(memory_space=pltpu.MemorySpace.HBM)
COPIES = 27


def compute(hist, states, cot, gain, wq, wo):
    n = 16 * S
    return pl.pallas_call(
        kernel,
        out_shape=(
            jax.ShapeDtypeStruct((n, D), bf16),
            jax.ShapeDtypeStruct((n, D), bf16),
            jax.ShapeDtypeStruct((12, 3, 3, 64), f32),
            jax.ShapeDtypeStruct((3, 12, 64), f32),
            jax.ShapeDtypeStruct((1, 12), f32),
        ),
        in_specs=[pl.BlockSpec(memory_space=pltpu.SMEM)] + [HBM] * 5,
        out_specs=(VMEM,) * 5,
        scratch_shapes=[
            pltpu.VMEM((n, D), bf16),
            pltpu.VMEM((n, D), bf16),
            pltpu.VMEM((D,), f32),
            pltpu.VMEM((4, 4, 256, D), bf16),
            pltpu.VMEM((n, D), bf16),
            pltpu.VMEM((n, D), bf16),
            pltpu.VMEM((n, 128), f32),
            pltpu.VMEM((2, NB, S, 256), bf16),
            pltpu.VMEM((2, NB, S, 256), bf16),
            pltpu.VMEM((2, NB, 256, 256), bf16),
            pltpu.VMEM((2, NB, 256, 256), bf16),
            pltpu.VMEM((n, 256), bf16),
            pltpu.VMEM((n, D), bf16),
            pltpu.VMEM((n, D), f32),
            pltpu.VMEM((n, D), f32),
            pltpu.VMEM((2, D, 384), bf16),
            pltpu.VMEM((D, 384), bf16),
            pltpu.VMEM((D, 384), bf16),
            pltpu.VMEM((3, 192, 384), bf16),
            pltpu.VMEM((192, 384), bf16),
            pltpu.VMEM((3, 48, 384), bf16),
            pltpu.VMEM((2, 48, 384), bf16),
            pltpu.VMEM((48, 384), bf16),
            pltpu.VMEM((2, 48, 384), bf16),
            pltpu.VMEM((4, 16, D), f32),
            pltpu.VMEM((5, 8, D), f32),
            pltpu.VMEM((11, 8, D), f32),
            pltpu.SemaphoreType.DMA((5,)),
            pltpu.SemaphoreType.DMA((COPIES,)),
            pltpu.SemaphoreType.DMA((COPIES,)),
        ],
        compiler_params=pltpu.CompilerParams(
            vmem_limit_bytes=40 * 2**20, collective_id=0, has_side_effects=True
        ),
    )(*[pltpu.with_memory_space_constraint(v, pltpu.HBM) for v in (hist, states, cot, gain, wq, wo)])


def put_kernel(*refs):
    n = len(refs) // 2
    sem = refs[-1]
    copies = [pltpu.make_async_copy(refs[k], refs[n + k], sem.at[k]) for k in range(n)]
    for c in copies:
        c.start()
    for c in copies:
        c.wait()


def put(arrays):
    return pl.pallas_call(
        put_kernel,
        out_shape=tuple(jax.ShapeDtypeStruct(a.shape, a.dtype) for a in arrays),
        in_specs=[VMEM] * len(arrays),
        out_specs=(HBM,) * len(arrays),
        scratch_shapes=[pltpu.SemaphoreType.DMA((len(arrays),))],
        compiler_params=pltpu.CompilerParams(vmem_limit_bytes=2**20),
    )(*arrays)


def body(states, hist_len, norm_gain, qkv_weight, output_weight, cotangent):
    wq = jnp.transpose(qkv_weight, (1, 2, 3, 0)).reshape(3, 192, D)
    wo = output_weight.reshape(192, D)
    attended, gstates, gq, go, gg = put(
        compute(hist_len, states.reshape(-1, D), cotangent.reshape(-1, D), norm_gain, wq, wo)
    )
    shape = states.shape
    return (
        attended.reshape(shape),
        gstates.reshape(shape),
        gq,
        jnp.transpose(go, (0, 2, 1)),
        gg.reshape(12),
    )


def solution(mesh):
    placed = (
        P("dp", None, None),
        P("dp"),
        P(),
        P(None, None, "mp", None),
        P("mp", None, None),
        P("dp", None, None),
    )
    return jax.shard_map(
        body,
        mesh=mesh,
        in_specs=placed,
        out_specs=(
            P("dp", None, None),
            P("dp", None, None),
            P("dp", None, "mp", None),
            P("mp", None, "dp"),
            P("dp"),
        ),
        check_vma=False,
    )
```

```python
import jax
import jax.numpy as jnp
from jax import lax
from jax.experimental import pallas as pl
from jax.experimental.pallas import tpu as pltpu
from jax.sharding import PartitionSpec as P

S = 80
D = 768
NB = 4
R = NB * S
PER = 16 // NB
f32 = jnp.float32
bf16 = jnp.bfloat16
PARTS = ((3,), (0,), (1,), (2,), (4, 5))
MESH = pl.DeviceIdType.MESH


def dot(a, b, ca, cb):
    return lax.dot_general(a, b, (((ca,), (cb,)), ((), ())), preferred_element_type=f32)


def nt(a, b):
    return dot(a, b, 1, 1)


def nn(a, b):
    return dot(a, b, 1, 0)


def tn(a, b):
    return dot(a, b, 0, 0)


def block_rows(t):
    return pl.ds(pl.multiple_of(lax.rem(t, PER) * R, R), R)


def prologue(i, states, cot, hist, gain, normed, mcot, inv):
    for j in range(NB):
        b = i * NB + j
        r = pl.ds(pl.multiple_of(b * S, S), S)
        x = states[r, :].astype(f32)
        iv = lax.rsqrt(jnp.mean(x * x, axis=-1, keepdims=True) + 1e-6)
        inv[r, :] = jnp.broadcast_to(iv, (S, 128))
        normed[r, :] = ((x * iv) * gain[...].reshape(1, D)).astype(bf16)
        keep = lax.broadcasted_iota(jnp.int32, (S, D), 0) < 4 * hist[b]
        mcot[r, :] = jnp.where(keep, cot[r, :].astype(f32), 0.0).astype(bf16)


def fill(t, w, normed, mcot, kb, vb, qs, dcs):
    slot = t // PER
    buf = lax.rem(t, 2)
    rows = block_rows(t)
    low = lax.broadcasted_iota(jnp.int32, (S, 128), 1) < 64

    def stack(ref, j, v):
        lo = v[:, 0:128]
        ref[buf, j, 0:S, 0:128] = jnp.where(low, lo, 0.0).astype(bf16)
        ref[buf, j, S : 2 * S, 0:128] = jnp.where(low, 0.0, lo).astype(bf16)
        ref[buf, j, 2 * S : 3 * S, 128:256] = v[:, 128:256].astype(bf16)

    for c in range(4):
        v = nt((mcot if c == 3 else normed)[rows, :], w[slot, c])
        for j in range(NB):
            one = v[j * S : (j + 1) * S]
            if c == 0:
                stack(qs, j, one)
            elif c == 3:
                stack(dcs, j, one)
            else:
                (kb if c == 1 else vb)[buf, j] = one.astype(bf16)


def push_part(t, n, w, ctx, gproj, att, gn):
    slot = t // PER
    rows = block_rows(t)
    c = slice(256 * (n % 3), 256 * (n % 3) + 256)
    if n < 3:
        att[rows, c] += nn(ctx[rows, :], w[slot, 3, :, c])
    else:
        gn[rows, c] += nn(gproj[rows, :], w[slot, 0:3, :, c].reshape(768, 256))


def push(t, *refs):
    for n in range(6):
        push_part(t, n, *refs)


def attend(t, hist, w, kb, vb, qs, dcs, ctx, gproj, att, gn):
    buf = lax.rem(t, 2)
    i = lax.rem(t, PER)
    row = lax.broadcasted_iota(jnp.int32, (S, 256), 0)
    low = lax.broadcasted_iota(jnp.int32, (S, 128), 1) < 64
    before = t - 1 + jnp.where(t == 0, PER, 0)
    pb, ds = [], []
    for n in PARTS[0]:
        push_part(before, n, w, ctx, gproj, att, gn)
    for j in range(NB):
        st = nt(kb[buf, j], qs[buf, j])
        dp = nt(vb[buf, j], dcs[buf, j])
        for n in PARTS[j + 1]:
            push_part(before, n, w, ctx, gproj, att, gn)
        x = jnp.where(row < 4 * hist[i * NB + j], st, -1e30)
        e = jnp.exp(x - jnp.max(x, axis=0, keepdims=True))
        p = e * (1.0 / jnp.sum(e, axis=0, keepdims=True))
        pb.append(p.astype(bf16))
        pd = p * dp
        ds.append((pd - p * jnp.sum(pd, axis=0, keepdims=True)).astype(bf16))

    def heads(o):
        two = jnp.where(low, o[0:S, 0:128], o[S : 2 * S, 0:128])
        return two.astype(bf16), o[2 * S : 3 * S, 128:256].astype(bf16)

    for j in range(NB):
        rr = pl.ds(pl.multiple_of((i * NB + j) * S, S), S)
        ctx[rr, 0:128], ctx[rr, 128:256] = heads(tn(pb[j], vb[buf, j]))
        gproj[rr, 512:768] = nn(pb[j], dcs[buf, j]).astype(bf16)
        gproj[rr, 0:128], gproj[rr, 128:256] = heads(tn(ds[j], kb[buf, j]))
        gproj[rr, 256:512] = nn(ds[j], qs[buf, j]).astype(bf16)


def wgrads(normed, mcot, ctx, gproj, gs):
    def body(t, _):
        c = pl.ds(pl.multiple_of(t * 256, 256), 256)
        g = tn(normed[:, c], gproj[...])
        o = tn(mcot[:, c], ctx[...])
        gs[0, c, 0:128] = g[:, 0:128].astype(bf16)
        gs[0, c, 128:256] = g[:, 256:384].astype(bf16)
        gs[0, c, 256:384] = g[:, 512:640].astype(bf16)
        gs[1, c, 0:128] = o[:, 0:128].astype(bf16)
        gs[1, c, 128:256] = (g[:, 128:256] + pltpu.roll(g[:, 384:512], 64, 1)).astype(bf16)
        gs[1, c, 256:384] = (g[:, 640:768] + pltpu.roll(o[:, 128:256], 64, 1)).astype(bf16)
        return 0

    lax.fori_loop(0, 3, body, 0)


def local_gain(states, inv, gn, gg):
    gg[...] = jnp.zeros_like(gg)

    def body(b, _):
        r = pl.ds(pl.multiple_of(b * S, S), S)
        t = gn[r, :] * (states[r, :].astype(f32) * inv[r, 0:1])
        gg[...] += jnp.sum(t.reshape(S // 8, 8, D), axis=0)
        return 0

    lax.fori_loop(0, 16, body, 0)


def epilogue(i, states, gain, mcot, inv, att, gn, attended, gstates):
    for j in range(NB):
        r = pl.ds(pl.multiple_of((i * NB + j) * S, S), S)
        x = states[r, :].astype(f32)
        iv = inv[r, 0:1]
        attended[r, :] = (x + att[r, :]).astype(bf16)
        u = x * iv
        gu = gn[r, :] * gain[...].reshape(1, D)
        m = iv * jnp.mean(gu * u, axis=-1, keepdims=True)
        gstates[r, :] = (mcot[r, :].astype(f32) + (iv * gu - u * m)).astype(bf16)


def kernel(
    hist, states_hbm, cot_hbm, gain_hbm, wq_hbm, wo_hbm,
    attended, gstates, gq_out, go_out, gg_out,
    states, cot, gain, w, normed, mcot, inv, kb, vb, qs, dcs, ctx, gproj, att, gn,
    gs, ra, sb, rb, sc, rc, sd, rd, fin, rows, gg, gb,
    load_sem, send_sem, recv_sem,
):
    dp, zl = lax.axis_index("dp"), lax.axis_index("mp")
    x, y, zh, core = dp // 16, lax.rem(dp // 4, 4), lax.rem(dp // 2, 2), lax.rem(dp, 2)
    z = zh * 4 + zl

    def dev(x, y, z, core):
        return (((x * 4 + y) * 2 + z // 4) * 2 + core, lax.rem(z, 4))

    def at_z(k):
        return dev(x, y, lax.rem(z + k, 8), core)

    up, down, up2, down2, far = at_z(1), at_z(7), at_z(2), at_z(6), at_z(4)
    twin = dev(x, y, z, 1 - core)
    xs = [dev(lax.rem(x + k, 4), y, z, core) for k in (1, 2, 3)]
    ys = [dev(x, lax.rem(y + k, 4), z, core) for k in (1, 2, 3)]

    def load(k, src, dst):
        return pltpu.make_async_copy(src, dst, load_sem.at[k])

    w_loads = [
        load(0, wq_hbm, w.at[0, pl.ds(0, 3), pl.ds(0, 192), :]),
        load(1, wo_hbm, w.at[0, 3, pl.ds(0, 192), :]),
    ]
    gain_load = load(2, gain_hbm, gain)
    x_loads = []
    for i in range(PER):
        r = pl.ds(i * R, R)
        x_loads.append(load(3 + 2 * i, states_hbm.at[r, :], states.at[r, :]))
        x_loads.append(load(4 + 2 * i, cot_hbm.at[r, :], cot.at[r, :]))

    def start(cs):
        for c in cs:
            c.start()

    def wait(cs):
        for c in cs:
            c.wait()

    start(w_loads)
    barrier = pltpu.get_barrier_semaphore()
    peers = [up, down, up2, down2, far, twin] + xs + ys
    for p in peers:
        pl.semaphore_signal(barrier, inc=1, device_id=p, device_id_type=MESH)
    gain_load.start()
    start(x_loads)

    count = [0]

    def remote(src, dst, device):
        k = count[0]
        count[0] += 1
        return pltpu.make_async_remote_copy(
            src_ref=src, dst_ref=dst, send_sem=send_sem.at[k], recv_sem=recv_sem.at[k],
            device_id=device, device_id_type=MESH,
        )

    def part(slot, first, n, at=0, size=192):
        return w.at[slot, pl.ds(first, n), pl.ds(at, size), :]

    def head(slot, k):
        return part(slot, c2, 2, 64 * k, 64)

    c2 = 2 * core
    near = [
        remote(head(0, 0), head(1, 0), up), remote(head(0, 0), head(1, 2), down),
        remote(head(0, 1), head(1, 1), up), remote(head(0, 1), head(2, 0), down),
        remote(head(0, 2), head(2, 2), up), remote(head(0, 2), head(2, 1), down),
    ]
    opposite = [
        remote(part(0, c2, 1), part(3, c2, 1), up2),
        remote(part(0, c2 + 1, 1), part(3, c2 + 1, 1), down2),
    ]
    pass_1 = [remote(head(1, k), head(1, k), twin) for k in (0, 2, 1)]
    pass_2 = remote(part(2, c2, 2), part(2, c2, 2), twin)
    pass_3 = remote(part(3, c2, 2), part(3, c2, 2), twin)

    g_a, n_a = remote(gs.at[1 - core], ra, twin), remote(gg.at[0], gb.at[0], twin)
    g_b, n_b, g_c, n_c = [], [], [], []
    for k in (1, 2, 3):
        chunk = pl.ds(pl.multiple_of(lax.rem(x + k, 4) * 192, 192), 192)
        g_b.append(remote(sb.at[chunk, :], rb.at[k - 1], xs[k - 1]))
        n_b.append(remote(gg.at[1], gb.at[k], xs[k - 1]))
        chunk = pl.ds(pl.multiple_of(lax.rem(y + k, 4) * 48, 48), 48)
        g_c.append(remote(sc.at[chunk, :], rc.at[k - 1], ys[k - 1]))
        n_c.append(remote(gg.at[2], gb.at[3 + k], ys[k - 1]))
    d_all = [remote(sd.at[0], rd, far), remote(gg.at[3], gb.at[7], far)]
    e_all = [remote(sd.at[1], fin.at[core], twin)]
    e_all += [remote(gg.at[4], gb.at[8 + k], d) for k, d in enumerate((up, down, up2))]

    for p in range(4):
        w[0, p, 192:256, :] = jnp.zeros((64, D), bf16)
    wait(w_loads)
    pl.semaphore_wait(barrier, len(peers))
    start(near)
    start(opposite)
    for s in range(1, 4):
        for p in range(4):
            w[s, p, 192:256, :] = jnp.zeros((64, D), bf16)
    for r in (qs, dcs, ctx, gproj, att, gn):
        r[...] = jnp.zeros_like(r)
    gain_load.wait()
    wait(x_loads)

    pro = (states, cot, hist, gain, normed, mcot, inv)
    fil = (w, normed, mcot, kb, vb, qs, dcs)
    atn = (hist, w, kb, vb, qs, dcs, ctx, gproj, att, gn)
    epi = (states, gain, mcot, inv, att, gn, attended, gstates)

    prologue(0, *pro)
    fill(0, *fil)
    prologue(1, *pro)

    def early(t, _):
        attend(t, *atn)
        fill(t + 1, *fil)
        prologue(jnp.minimum(t + 2, PER - 1), *pro)
        return 0

    lax.fori_loop(0, PER - 1, early, 0)
    wait(near[0:2])
    start(pass_1[0:2])
    attend(PER - 1, *atn)
    wgrads(normed, mcot, ctx, gproj, gs)
    near[2].wait()
    pass_1[2].start()
    g_a.start()
    wait(pass_1)
    fill(PER, *fil)

    def step(t, _):
        @pl.when(t == 7)
        def _():
            pass_2.wait()

        @pl.when(t == 11)
        def _():
            pass_3.wait()

        attend(t, *atn)
        fill(t + 1, *fil)

        @pl.when(t == 4)
        def _():
            local_gain(states, inv, gn, gg.at[0])
            wait(near[3:6])
            pass_2.start()

        @pl.when(t == 5)
        def _():
            n_a.start()
            g_a.wait()
            sb[...] = (gs[core].astype(f32) + ra[...].astype(f32)).astype(bf16)

        @pl.when(t == 6)
        def _():
            start(g_b)
            n_a.wait()
            gg[1] = gg[0] + gb[0]

        @pl.when(t == 7)
        def _():
            start(n_b)

        @pl.when(t == 9)
        def _():
            wait(g_b)
            wait(n_b)
            own = sb[pl.ds(pl.multiple_of(x * 192, 192), 192), :].astype(f32)
            for k in range(3):
                own += rb[k].astype(f32)
            sc[...] = own.astype(bf16)
            gg[2] = gg[1] + (gb[1] + gb[2] + gb[3])
            wait(opposite)
            pass_3.start()

        @pl.when(t == 10)
        def _():
            start(g_c)
            start(n_c)

        @pl.when(t == 11)
        def _():
            wait(g_c)
            wait(n_c)
            own = sc[pl.ds(pl.multiple_of(y * 48, 48), 48), :].astype(f32)
            for k in range(3):
                own += rc[k].astype(f32)
            sd[0] = own.astype(bf16)
            gg[3] = gg[2] + (gb[4] + gb[5] + gb[6])

        @pl.when(t == 12)
        def _():
            start(d_all)

        return 0

    lax.fori_loop(PER, 3 * PER + 1, step, 0)

    def late(t, _):
        attend(t, *atn)
        fill(t + 1, *fil)
        epilogue(lax.rem(t - 1, PER), *epi)

        @pl.when(t == 3 * PER + 1)
        def _():
            wait(d_all)
            both = (sd[0].astype(f32) + rd[...].astype(f32)).astype(bf16)
            sd[1] = both
            fin[core] = both
            gg[4] = gg[3] + gb[7]

        return 0

    lax.fori_loop(3 * PER + 1, 4 * PER - 1, late, 0)
    start(e_all)
    attend(4 * PER - 1, *atn)
    epilogue(PER - 2, *epi)
    wait(e_all)
    push(4 * PER - 1, w, ctx, gproj, att, gn)
    total = gg[4] + (gb[8] + gb[9] + gb[10])
    total = jnp.broadcast_to(jnp.sum(total, axis=0, keepdims=True), (8, D))
    gg_out[...] = pltpu.roll(total, lax.rem(D - 12 * dp, D), 1)[0:1, 0:12]
    for h in range(2):
        part_h = fin[h].astype(f32)
        for q in range(4):
            rows[q, 0:12, 384 * h : 384 * h + 384] = part_h[12 * q : 12 * q + 12]
    mine = rows[2 * zh + core, 0:12, :]
    for r in range(12):
        one = mine[r : r + 1]
        for c in range(3):
            at = 512 + 64 * c
            gq_out[r, c, 0:1, :] = one[:, 128 * c : 128 * c + 64]
            gq_out[r, c, 1:2, :] = one[:, 128 * c + 64 : 128 * c + 128]
            gq_out[r, c, 2:3, :] = one[:, at : at + 64]
    go_out[0] = mine[:, 384:448]
    go_out[1] = mine[:, 448:512]
    go_out[2] = mine[:, 704:768]
    epilogue(PER - 1, *epi)


VMEM = pl.BlockSpec(memory_space=pltpu.VMEM)
HBM = pl.BlockSpec(memory_space=pltpu.MemorySpace.HBM)
COPIES = 33


def in_hbm(*arrays):
    return [pltpu.with_memory_space_constraint(a, pltpu.HBM) for a in arrays]


def compute(*args):
    n = 16 * S

    def rows_of(width, kind, *lead):
        return pltpu.VMEM((*lead, n, width), kind)

    return pl.pallas_call(
        kernel,
        out_shape=(
            jax.ShapeDtypeStruct((n, D), bf16),
            jax.ShapeDtypeStruct((n, D), bf16),
            jax.ShapeDtypeStruct((12, 3, 3, 64), f32),
            jax.ShapeDtypeStruct((3, 12, 64), f32),
            jax.ShapeDtypeStruct((1, 12), f32),
        ),
        in_specs=[pl.BlockSpec(memory_space=pltpu.SMEM)] + [HBM] * 5,
        out_specs=(VMEM,) * 5,
        scratch_shapes=[
            rows_of(D, bf16),
            rows_of(D, bf16),
            pltpu.VMEM((D,), f32),
            pltpu.VMEM((4, 4, 256, D), bf16),
            rows_of(D, bf16),
            rows_of(D, bf16),
            rows_of(128, f32),
            pltpu.VMEM((2, NB, S, 256), bf16),
            pltpu.VMEM((2, NB, S, 256), bf16),
            pltpu.VMEM((2, NB, 256, 256), bf16),
            pltpu.VMEM((2, NB, 256, 256), bf16),
            rows_of(256, bf16),
            rows_of(D, bf16),
            rows_of(D, f32),
            rows_of(D, f32),
            pltpu.VMEM((2, D, 384), bf16),
            pltpu.VMEM((D, 384), bf16),
            pltpu.VMEM((D, 384), bf16),
            pltpu.VMEM((3, 192, 384), bf16),
            pltpu.VMEM((192, 384), bf16),
            pltpu.VMEM((3, 48, 384), bf16),
            pltpu.VMEM((2, 48, 384), bf16),
            pltpu.VMEM((48, 384), bf16),
            pltpu.VMEM((2, 48, 384), bf16),
            pltpu.VMEM((4, 16, D), f32),
            pltpu.VMEM((5, 8, D), f32),
            pltpu.VMEM((11, 8, D), f32),
            pltpu.SemaphoreType.DMA((3 + 2 * PER,)),
            pltpu.SemaphoreType.DMA((COPIES,)),
            pltpu.SemaphoreType.DMA((COPIES,)),
        ],
        compiler_params=pltpu.CompilerParams(
            vmem_limit_bytes=44 * 2**20, collective_id=0, has_side_effects=True
        ),
    )(*in_hbm(*args))


def put_kernel(*refs):
    n = len(refs) // 2
    sem = refs[-1]
    copies = [pltpu.make_async_copy(refs[k], refs[n + k], sem.at[k]) for k in range(n)]
    for c in copies:
        c.start()
    for c in copies:
        c.wait()


def put(arrays):
    return pl.pallas_call(
        put_kernel,
        out_shape=tuple(jax.ShapeDtypeStruct(a.shape, a.dtype) for a in arrays),
        in_specs=[VMEM] * len(arrays),
        out_specs=(HBM,) * len(arrays),
        scratch_shapes=[pltpu.SemaphoreType.DMA((len(arrays),))],
        compiler_params=pltpu.CompilerParams(vmem_limit_bytes=2**20),
    )(*arrays)


def body(states, hist_len, norm_gain, qkv_weight, output_weight, cotangent):
    wq = jnp.transpose(qkv_weight, (1, 2, 3, 0)).reshape(3, 192, D)
    wo = output_weight.reshape(192, D)
    attended, gstates, gq, go, gg = put(
        compute(hist_len, states.reshape(-1, D), cotangent.reshape(-1, D), norm_gain, wq, wo)
    )
    shape = states.shape
    return (
        attended.reshape(shape),
        gstates.reshape(shape),
        gq,
        jnp.transpose(go, (0, 2, 1)),
        gg.reshape(12),
    )


def solution(mesh):
    placed = (
        P("dp", None, None),
        P("dp"),
        P(),
        P(None, None, "mp", None),
        P("mp", None, None),
        P("dp", None, None),
    )
    return jax.shard_map(
        body,
        mesh=mesh,
        in_specs=placed,
        out_specs=(
            P("dp", None, None),
            P("dp", None, None),
            P("dp", None, "mp", None),
            P("mp", None, "dp"),
            P("dp"),
        ),
        check_vma=False,
    )
```

```python
import jax
import jax.numpy as jnp
from jax import lax
from jax.experimental import pallas as pl
from jax.experimental.pallas import tpu as pltpu
from jax.sharding import PartitionSpec as P

S = 80
D = 768
NB = 4
R = NB * S
PER = 16 // NB
f32 = jnp.float32
bf16 = jnp.bfloat16
PARTS = ((3,), (0,), (1,), (2,), (4, 5))
MESH = pl.DeviceIdType.MESH


def dot(a, b, ca, cb):
    return lax.dot_general(a, b, (((ca,), (cb,)), ((), ())), preferred_element_type=f32)


def nt(a, b):
    return dot(a, b, 1, 1)


def nn(a, b):
    return dot(a, b, 1, 0)


def tn(a, b):
    return dot(a, b, 0, 0)


def block_rows(t):
    return pl.ds(pl.multiple_of(lax.rem(t, PER) * R, R), R)


def prologue(i, states, cot, hist, gain, normed, mcot, inv):
    for j in range(NB):
        b = i * NB + j
        r = pl.ds(pl.multiple_of(b * S, S), S)
        x = states[r, :].astype(f32)
        iv = lax.rsqrt(jnp.mean(x * x, axis=-1, keepdims=True) + 1e-6)
        inv[r, :] = jnp.broadcast_to(iv, (S, 128))
        normed[r, :] = ((x * iv) * gain[...].reshape(1, D)).astype(bf16)
        keep = lax.broadcasted_iota(jnp.int32, (S, D), 0) < 4 * hist[b]
        mcot[r, :] = jnp.where(keep, cot[r, :].astype(f32), 0.0).astype(bf16)


def fill(t, w, normed, mcot, kb, vb, qs, dcs):
    slot = t // PER
    buf = lax.rem(t, 2)
    rows = block_rows(t)
    low = lax.broadcasted_iota(jnp.int32, (S, 128), 1) < 64

    def stack(ref, j, v):
        lo = v[:, 0:128]
        ref[buf, j, 0:S, 0:128] = jnp.where(low, lo, 0.0).astype(bf16)
        ref[buf, j, S : 2 * S, 0:128] = jnp.where(low, 0.0, lo).astype(bf16)
        ref[buf, j, 2 * S : 3 * S, 128:256] = v[:, 128:256].astype(bf16)

    for c in range(4):
        v = nt((mcot if c == 3 else normed)[rows, :], w[slot, c])
        for j in range(NB):
            one = v[j * S : (j + 1) * S]
            if c == 0:
                stack(qs, j, one)
            elif c == 3:
                stack(dcs, j, one)
            else:
                (kb if c == 1 else vb)[buf, j] = one.astype(bf16)


def push_part(t, n, w, ctx, gproj, att, gn):
    slot = t // PER
    rows = block_rows(t)
    c = slice(256 * (n % 3), 256 * (n % 3) + 256)
    if n < 3:
        att[rows, c] += nn(ctx[rows, :], w[slot, 3, :, c])
    else:
        gn[rows, c] += nn(gproj[rows, :], w[slot, 0:3, :, c].reshape(768, 256))


def push(t, *refs):
    for n in range(6):
        push_part(t, n, *refs)


def attend(t, hist, w, kb, vb, qs, dcs, ctx, gproj, att, gn):
    buf = lax.rem(t, 2)
    i = lax.rem(t, PER)
    row = lax.broadcasted_iota(jnp.int32, (S, 256), 0)
    low = lax.broadcasted_iota(jnp.int32, (S, 128), 1) < 64
    before = t - 1 + jnp.where(t == 0, PER, 0)
    pb, ds = [], []
    for n in PARTS[0]:
        push_part(before, n, w, ctx, gproj, att, gn)
    for j in range(NB):
        st = nt(kb[buf, j], qs[buf, j])
        dp = nt(vb[buf, j], dcs[buf, j])
        for n in PARTS[j + 1]:
            push_part(before, n, w, ctx, gproj, att, gn)
        x = jnp.where(row < 4 * hist[i * NB + j], st, -1e30)
        e = jnp.exp(x - jnp.max(x, axis=0, keepdims=True))
        p = e * (1.0 / jnp.sum(e, axis=0, keepdims=True))
        pb.append(p.astype(bf16))
        pd = p * dp
        ds.append((pd - p * jnp.sum(pd, axis=0, keepdims=True)).astype(bf16))

    def heads(o):
        two = jnp.where(low, o[0:S, 0:128], o[S : 2 * S, 0:128])
        return two.astype(bf16), o[2 * S : 3 * S, 128:256].astype(bf16)

    for j in range(NB):
        rr = pl.ds(pl.multiple_of((i * NB + j) * S, S), S)
        ctx[rr, 0:128], ctx[rr, 128:256] = heads(tn(pb[j], vb[buf, j]))
        gproj[rr, 512:768] = nn(pb[j], dcs[buf, j]).astype(bf16)
        gproj[rr, 0:128], gproj[rr, 128:256] = heads(tn(ds[j], kb[buf, j]))
        gproj[rr, 256:512] = nn(ds[j], qs[buf, j]).astype(bf16)


def wgrads(normed, mcot, ctx, gproj, gs):
    def body(t, _):
        c = pl.ds(pl.multiple_of(t * 256, 256), 256)
        g = tn(normed[:, c], gproj[...])
        o = tn(mcot[:, c], ctx[...])
        gs[0, c, 0:128] = g[:, 0:128].astype(bf16)
        gs[0, c, 128:256] = g[:, 256:384].astype(bf16)
        gs[0, c, 256:384] = g[:, 512:640].astype(bf16)
        gs[1, c, 0:128] = o[:, 0:128].astype(bf16)
        gs[1, c, 128:256] = (g[:, 128:256] + pltpu.roll(g[:, 384:512], 64, 1)).astype(bf16)
        gs[1, c, 256:384] = (g[:, 640:768] + pltpu.roll(o[:, 128:256], 64, 1)).astype(bf16)
        return 0

    lax.fori_loop(0, 3, body, 0)


def local_gain(states, inv, gn, gg):
    gg[...] = jnp.zeros_like(gg)

    def body(b, _):
        r = pl.ds(pl.multiple_of(b * S, S), S)
        t = gn[r, :] * (states[r, :].astype(f32) * inv[r, 0:1])
        gg[...] += jnp.sum(t.reshape(S // 8, 8, D), axis=0)
        return 0

    lax.fori_loop(0, 16, body, 0)


def epilogue(i, states, gain, mcot, inv, att, gn, attended, gstates):
    for j in range(NB):
        r = pl.ds(pl.multiple_of((i * NB + j) * S, S), S)
        x = states[r, :].astype(f32)
        iv = inv[r, 0:1]
        attended[r, :] = (x + att[r, :]).astype(bf16)
        u = x * iv
        gu = gn[r, :] * gain[...].reshape(1, D)
        m = iv * jnp.mean(gu * u, axis=-1, keepdims=True)
        gstates[r, :] = (mcot[r, :].astype(f32) + (iv * gu - u * m)).astype(bf16)


def kernel(
    hist, states_hbm, cot_hbm, gain_hbm, wq_hbm, wo_hbm,
    attended, gstates, gq_out, go_out, gg_out,
    states, cot, gain, w, normed, mcot, inv, kb, vb, qs, dcs, ctx, gproj, att, gn,
    gs, ra, sb, rb, sc, rc, sd, rd, fin, rows, gg, gb,
    load_sem, send_sem, recv_sem,
):
    dp, zl = lax.axis_index("dp"), lax.axis_index("mp")
    x, y, zh, core = dp // 16, lax.rem(dp // 4, 4), lax.rem(dp // 2, 2), lax.rem(dp, 2)
    z = zh * 4 + zl

    def dev(x, y, z, core):
        return (((x * 4 + y) * 2 + z // 4) * 2 + core, lax.rem(z, 4))

    def at_z(k):
        return dev(x, y, lax.rem(z + k, 8), core)

    up, down, up2, down2, far = at_z(1), at_z(7), at_z(2), at_z(6), at_z(4)
    twin = dev(x, y, z, 1 - core)
    far_twin = dev(x, y, lax.rem(z + 4, 8), 1 - core)
    c1 = 1 - core
    first = [dev(lax.rem(x + k * c1, 4), lax.rem(y + k * core, 4), z, core) for k in (1, 2, 3)]
    second = [dev(lax.rem(x + k * core, 4), lax.rem(y + k * c1, 4), z, core) for k in (1, 2, 3)]
    one, two = x * c1 + y * core, x * core + y * c1
    column = [at_z(k) for k in range(1, 8)]

    def load(k, src, dst):
        return pltpu.make_async_copy(src, dst, load_sem.at[k])

    w_loads = [
        load(0, wq_hbm, w.at[0, pl.ds(0, 3), pl.ds(0, 192), :]),
        load(1, wo_hbm, w.at[0, 3, pl.ds(0, 192), :]),
    ]
    gain_load = load(2, gain_hbm, gain)
    x_loads = []
    for i in range(PER):
        r = pl.ds(i * R, R)
        x_loads.append(load(3 + 2 * i, states_hbm.at[r, :], states.at[r, :]))
        x_loads.append(load(4 + 2 * i, cot_hbm.at[r, :], cot.at[r, :]))

    def start(cs):
        for c in cs:
            c.start()

    def wait(cs):
        for c in cs:
            c.wait()

    start(w_loads)
    barrier = pltpu.get_barrier_semaphore()
    peers = [twin, far_twin] + column + first + second
    for p in peers:
        pl.semaphore_signal(barrier, inc=1, device_id=p, device_id_type=MESH)
    gain_load.start()
    start(x_loads)

    count = [0]

    def remote(src, dst, device):
        k = count[0]
        count[0] += 1
        return pltpu.make_async_remote_copy(
            src_ref=src, dst_ref=dst, send_sem=send_sem.at[k], recv_sem=recv_sem.at[k],
            device_id=device, device_id_type=MESH,
        )

    def part(slot, first, n, at=0, size=192):
        return w.at[slot, pl.ds(first, n), pl.ds(at, size), :]

    def head(slot, k):
        return part(slot, c2, 2, 64 * k, 64)

    c2 = 2 * core
    near = [
        remote(head(0, 0), head(1, 0), up), remote(head(0, 0), head(1, 2), down),
        remote(head(0, 1), head(1, 1), up), remote(head(0, 1), head(2, 0), down),
        remote(head(0, 2), head(2, 2), up), remote(head(0, 2), head(2, 1), down),
    ]
    opposite = [
        remote(part(0, c2, 1), part(3, c2, 1), up2),
        remote(part(0, c2 + 1, 1), part(3, c2 + 1, 1), down2),
    ]
    pass_1 = [remote(head(1, k), head(1, k), twin) for k in (0, 2, 1)]
    pass_2 = remote(part(2, c2, 2), part(2, c2, 2), twin)
    pass_3 = remote(part(3, c2, 2), part(3, c2, 2), twin)

    g_a, n_a = remote(gs.at[1 - core], ra, twin), remote(gg.at[0], gb.at[0], twin)
    g_b, n_b, g_c, n_c = [], [], [], []
    for k in (1, 2, 3):
        g_b.append(remote(sb.at[lax.rem(one + k, 4)], rb.at[k - 1], first[k - 1]))
        n_b.append(remote(gg.at[1], gb.at[k], first[k - 1]))
        g_c.append(remote(sc.at[lax.rem(two + k, 4)], rc.at[k - 1], second[k - 1]))
        n_c.append(remote(gg.at[2], gb.at[3 + k], second[k - 1]))
    g_d = [remote(sd, rd.at[k], p) for k, p in enumerate((far, twin, far_twin))]
    n_d = [remote(gg.at[3], gb.at[6 + k], p) for k, p in enumerate(column, 1)]

    for p in range(4):
        w[0, p, 192:256, :] = jnp.zeros((64, D), bf16)
    wait(w_loads)
    pl.semaphore_wait(barrier, len(peers))
    start(near)
    start(opposite)
    for s in range(1, 4):
        for p in range(4):
            w[s, p, 192:256, :] = jnp.zeros((64, D), bf16)
    for r in (qs, dcs, ctx, gproj, att, gn):
        r[...] = jnp.zeros_like(r)
    gain_load.wait()
    wait(x_loads)

    pro = (states, cot, hist, gain, normed, mcot, inv)
    fil = (w, normed, mcot, kb, vb, qs, dcs)
    atn = (hist, w, kb, vb, qs, dcs, ctx, gproj, att, gn)
    epi = (states, gain, mcot, inv, att, gn, attended, gstates)

    prologue(0, *pro)
    fill(0, *fil)
    prologue(1, *pro)

    def early(t, _):
        attend(t, *atn)
        fill(t + 1, *fil)
        prologue(jnp.minimum(t + 2, PER - 1), *pro)
        return 0

    lax.fori_loop(0, PER - 1, early, 0)
    wait(near[0:2])
    start(pass_1[0:2])
    attend(PER - 1, *atn)
    wgrads(normed, mcot, ctx, gproj, gs)
    near[2].wait()
    pass_1[2].start()
    g_a.start()
    wait(pass_1)
    fill(PER, *fil)

    def step(t, _):
        @pl.when(t == 7)
        def _():
            pass_2.wait()

        @pl.when(t == 11)
        def _():
            pass_3.wait()

        attend(t, *atn)
        fill(t + 1, *fil)

        @pl.when(t == 4)
        def _():
            g_a.wait()
            for i in range(4):
                for j in range(4):
                    r = slice(192 * i + 48 * j, 192 * i + 48 * j + 48)
                    both = gs[core, r, :].astype(f32) + ra[r, :].astype(f32)
                    sb[i * c1 + j * core, i * core + j * c1] = both.astype(bf16)
            local_gain(states, inv, gn, gg.at[0])
            start(g_b)
            n_a.start()
            wait(near[3:6])
            pass_2.start()

        @pl.when(t == 5)
        def _():
            n_a.wait()
            gg[1] = gg[0] + gb[0]

        @pl.when(t == 6)
        def _():
            start(n_b)

        @pl.when(t == 8)
        def _():
            wait(g_b)
            own = sb[one].astype(f32)
            for k in range(3):
                own += rb[k].astype(f32)
            sc[...] = own.astype(bf16)
            wait(n_b)
            gg[2] = gg[1] + (gb[1] + gb[2] + gb[3])
            start(g_c)
            start(n_c)

        @pl.when(t == 9)
        def _():
            wait(opposite)
            pass_3.start()

        @pl.when(t == 10)
        def _():
            wait(g_c)
            own = sc[two].astype(f32)
            for k in range(3):
                own += rc[k].astype(f32)
            sd[...] = own.astype(bf16)
            wait(n_c)
            gg[3] = gg[2] + (gb[4] + gb[5] + gb[6])
            start(g_d)
            start(n_d)

        return 0

    lax.fori_loop(PER, 3 * PER + 1, step, 0)

    def late(t, _):
        attend(t, *atn)
        fill(t + 1, *fil)
        epilogue(lax.rem(t - 1, PER), *epi)
        return 0

    lax.fori_loop(3 * PER + 1, 4 * PER - 1, late, 0)
    attend(4 * PER - 1, *atn)
    epilogue(PER - 2, *epi)
    push(4 * PER - 1, w, ctx, gproj, att, gn)
    wait(g_d)
    wait(n_d)
    total = gg[3]
    for k in range(1, 8):
        total += gb[6 + k]
    total = jnp.broadcast_to(jnp.sum(total, axis=0, keepdims=True), (8, D))
    gg_out[...] = pltpu.roll(total, lax.rem(D - 12 * dp, D), 1)[0:1, 0:12]
    fin[core] = sd[...].astype(f32) + rd[0].astype(f32)
    fin[c1] = rd[1].astype(f32) + rd[2].astype(f32)
    for h in range(2):
        for q in range(4):
            rows[q, 0:12, 384 * h : 384 * h + 384] = fin[h, 12 * q : 12 * q + 12, :]
    mine = rows[2 * zh + core, 0:12, :]
    for r in range(12):
        line = mine[r : r + 1]
        for c in range(3):
            at = 512 + 64 * c
            gq_out[r, c, 0:1, :] = line[:, 128 * c : 128 * c + 64]
            gq_out[r, c, 1:2, :] = line[:, 128 * c + 64 : 128 * c + 128]
            gq_out[r, c, 2:3, :] = line[:, at : at + 64]
    go_out[0] = mine[:, 384:448]
    go_out[1] = mine[:, 448:512]
    go_out[2] = mine[:, 704:768]
    epilogue(PER - 1, *epi)


VMEM = pl.BlockSpec(memory_space=pltpu.VMEM)
HBM = pl.BlockSpec(memory_space=pltpu.MemorySpace.HBM)
COPIES = 37


def in_hbm(*arrays):
    return [pltpu.with_memory_space_constraint(a, pltpu.HBM) for a in arrays]


def compute(*args):
    n = 16 * S

    def rows_of(width, kind, *lead):
        return pltpu.VMEM((*lead, n, width), kind)

    return pl.pallas_call(
        kernel,
        out_shape=(
            jax.ShapeDtypeStruct((n, D), bf16),
            jax.ShapeDtypeStruct((n, D), bf16),
            jax.ShapeDtypeStruct((12, 3, 3, 64), f32),
            jax.ShapeDtypeStruct((3, 12, 64), f32),
            jax.ShapeDtypeStruct((1, 12), f32),
        ),
        in_specs=[pl.BlockSpec(memory_space=pltpu.SMEM)] + [HBM] * 5,
        out_specs=(VMEM,) * 5,
        scratch_shapes=[
            rows_of(D, bf16),
            rows_of(D, bf16),
            pltpu.VMEM((D,), f32),
            pltpu.VMEM((4, 4, 256, D), bf16),
            rows_of(D, bf16),
            rows_of(D, bf16),
            rows_of(128, f32),
            pltpu.VMEM((2, NB, S, 256), bf16),
            pltpu.VMEM((2, NB, S, 256), bf16),
            pltpu.VMEM((2, NB, 256, 256), bf16),
            pltpu.VMEM((2, NB, 256, 256), bf16),
            rows_of(256, bf16),
            rows_of(D, bf16),
            rows_of(D, f32),
            rows_of(D, f32),
            pltpu.VMEM((2, D, 384), bf16),
            pltpu.VMEM((D, 384), bf16),
            pltpu.VMEM((4, 4, 48, 384), bf16),
            pltpu.VMEM((3, 4, 48, 384), bf16),
            pltpu.VMEM((4, 48, 384), bf16),
            pltpu.VMEM((3, 48, 384), bf16),
            pltpu.VMEM((48, 384), bf16),
            pltpu.VMEM((3, 48, 384), bf16),
            pltpu.VMEM((2, 48, 384), f32),
            pltpu.VMEM((4, 16, D), f32),
            pltpu.VMEM((4, 8, D), f32),
            pltpu.VMEM((14, 8, D), f32),
            pltpu.SemaphoreType.DMA((3 + 2 * PER,)),
            pltpu.SemaphoreType.DMA((COPIES,)),
            pltpu.SemaphoreType.DMA((COPIES,)),
        ],
        compiler_params=pltpu.CompilerParams(
            vmem_limit_bytes=44 * 2**20, collective_id=0, has_side_effects=True
        ),
    )(*in_hbm(*args))


def put_kernel(*refs):
    n = len(refs) // 2
    sem = refs[-1]
    copies = [pltpu.make_async_copy(refs[k], refs[n + k], sem.at[k]) for k in range(n)]
    for c in copies:
        c.start()
    for c in copies:
        c.wait()


def put(arrays):
    return pl.pallas_call(
        put_kernel,
        out_shape=tuple(jax.ShapeDtypeStruct(a.shape, a.dtype) for a in arrays),
        in_specs=[VMEM] * len(arrays),
        out_specs=(HBM,) * len(arrays),
        scratch_shapes=[pltpu.SemaphoreType.DMA((len(arrays),))],
        compiler_params=pltpu.CompilerParams(vmem_limit_bytes=2**20),
    )(*arrays)


def body(states, hist_len, norm_gain, qkv_weight, output_weight, cotangent):
    wq = jnp.transpose(qkv_weight, (1, 2, 3, 0)).reshape(3, 192, D)
    wo = output_weight.reshape(192, D)
    attended, gstates, gq, go, gg = put(
        compute(hist_len, states.reshape(-1, D), cotangent.reshape(-1, D), norm_gain, wq, wo)
    )
    shape = states.shape
    return (
        attended.reshape(shape),
        gstates.reshape(shape),
        gq,
        jnp.transpose(go, (0, 2, 1)),
        gg.reshape(12),
    )


def solution(mesh):
    placed = (
        P("dp", None, None),
        P("dp"),
        P(),
        P(None, None, "mp", None),
        P("mp", None, None),
        P("dp", None, None),
    )
    return jax.shard_map(
        body,
        mesh=mesh,
        in_specs=placed,
        out_specs=(
            P("dp", None, None),
            P("dp", None, None),
            P("dp", None, "mp", None),
            P("mp", None, "dp"),
            P("dp"),
        ),
        check_vma=False,
    )
```
